128 devices in a mesh: leaf: 16 (over y, z), front: 8 (over x, core).
Axes of the slice: x: 4, y: 4, z: 4, core: 2. Of those that a mesh axis runs over, the one named last changes fastest.
Arguments:
- app_rhs: float32 [98304, 128], P(('leaf', 'front')), may hold values from -6 to 6
- pivot_source: int32 [98304], P(('leaf', 'front')), may hold values from 0 to 98303, as said below
- row_owner: int32 [98304], P(('leaf', 'front')), may hold values from 0 to 98303, as said below
- leaf_inverse: float32 [16, 8, 384, 3072], P('leaf', 'front'), may hold values from -1 to 2, as said below
- leaf_coupling: float32 [16, 8, 384, 2048], P('leaf', 'front'), may hold values from -0.054126587 to 0.054126587
- sep1_inverse: float32 [16, 8, 128, 2048], P('leaf', 'front'), may hold values from -1 to 2, as said below
- sep1_coupling: float32 [16, 8, 128, 4096], P('leaf', 'front'), may hold values from -0.06629126 to 0.06629126
- sep2_inverse: float32 [16, 8, 128, 4096], P('leaf', 'front'), may hold values from -1 to 2, as said below
- sep2_coupling: float32 [16, 8, 128, 8192], P('leaf', 'front'), may hold values from -0.046875 to 0.046875
- sep3_inverse: float32 [16, 8, 128, 8192], P('leaf', 'front'), may hold values from -1 to 2, as said below
Outputs:
- solution: float32 [98304, 128], P(('leaf', 'front'))
The draws below stay inside these ranges and needn't reach their ends.
Inputs may be any that keep to these rules, and one draw needn't show every extreme that they name: `pivot_source`: A permutation. Row e of pivot_rhs comes from a device's block of 768 application rows; one block's rows go to at most 64 blocks of pivot rows, at most 15 rows from one block to one block, and some pair of blocks carries exactly 15 rows. The inverse of pivot_source: pivot_source[row_owner[i]] = i. `leaf_inverse`: each front's matrix is the identity plus dense entries of magnitude at most 2 / sqrt of the front's pivot rows. `sep1_inverse`: as leaf_inverse. `sep2_inverse`: as leaf_inverse. `sep3_inverse`: as leaf_inverse.
All inputs are finite; a program needn't handle non-finite values.
Results may differ from the reference program's by a relative error of at most 0.00011.
Values sent between devices are 32-bit elements; how exact they have to be, the bound alone decides.
No kernel may reach another device: no remote copies, remote signals or barrier semaphores. Data moves between devices by JAX's collectives and lax.ppermute only.
A program may use at most 128 MiB of HBM per device.

```python
import jax
import jax.numpy as jnp
from jax import lax

NRHS = 128
LEAF_PIV = 384
SEP_PIV = 128
ROWS_DEV = 768
FANOUT = 64
SPREAD = 3
NROWS = 98304
LEAF_FRONT = 3072
SEP1 = 2048
SEP2 = 4096
SEP3 = 8192
N_LEAF = 16
N_FRONT = 8


def route_tables(key):
    base_key = jax.random.fold_in(key, 7)
    keys_all = jax.random.split(base_key, 6)
    device_count = N_LEAF * N_FRONT
    row_count = ROWS_DEV
    mean_rows = ROWS_DEV // FANOUT
    labels = jax.random.permutation(keys_all[0], device_count)
    turns = jax.random.permutation(keys_all[1], device_count)
    shifts = jax.random.permutation(keys_all[2], device_count)[:FANOUT]
    offsets = jax.random.randint(keys_all[3], (FANOUT // 2,), 0, SPREAD + 1)
    offsets = offsets.at[0].set(SPREAD)
    weights = jnp.stack([mean_rows + offsets, mean_rows - offsets], axis=1).reshape(FANOUT)
    bucket_ends = jnp.cumsum(weights)
    slot_index = jnp.arange(row_count, dtype=jnp.int32)
    bucket = jnp.sum((slot_index[:, None] >= bucket_ends[None, :]).astype(jnp.int32), axis=1)
    label_of = (turns[:, None] + shifts[bucket][None, :]) % device_count
    target = jnp.argsort(labels)[label_of].astype(jnp.int32)
    local_order = jax.vmap(lambda sub_key: jax.random.permutation(sub_key, row_count))(jax.random.split(keys_all[4], device_count))
    app_row = jnp.arange(device_count, dtype=jnp.int32)[:, None] * row_count + local_order.astype(jnp.int32)
    priority = jax.random.permutation(keys_all[5], device_count * row_count).reshape(device_count, row_count).astype(jnp.int32)
    scores = (target * (device_count * row_count) + priority).reshape(-1)
    sorted_items = jnp.argsort(scores, stable=True)
    source_rows = app_row.reshape(-1)[sorted_items].astype(jnp.int32)
    owner_rows = jnp.zeros(device_count * row_count, jnp.int32).at[source_rows].set(jnp.arange(device_count * row_count, dtype=jnp.int32))
    return (source_rows, owner_rows)


def draw_pivot_source(key, part):
    return route_tables(key)[0]


def draw_row_owner(key, part):
    return route_tables(key)[1]


def draw_front(key, group_size, pivot_rows, width):
    full_shape = (N_LEAF, N_FRONT, pivot_rows, width)
    leaf_axis = jnp.arange(N_LEAF)[:, None, None, None]
    front_axis = jnp.arange(N_FRONT)[None, :, None, None]
    pivot_axis = jnp.arange(pivot_rows)[None, None, :, None]
    column_axis = jnp.arange(width)[None, None, None, :]
    diagonal_col = front_axis * (group_size * pivot_rows) + leaf_axis % group_size * pivot_rows + pivot_axis
    identity = (column_axis == diagonal_col).astype(jnp.float32)
    jitter = jnp.clip(jax.random.normal(key, full_shape, jnp.float32), -4.0, 4.0)
    return identity + 0.5 * jitter / width ** 0.5


def draw_leaf_inverse(key, part):
    return draw_front(jax.random.fold_in(key, 11), 1, LEAF_PIV, LEAF_FRONT)


def draw_sep1_inverse(key, part):
    return draw_front(jax.random.fold_in(key, 12), 2, SEP_PIV, SEP1)


def draw_sep2_inverse(key, part):
    return draw_front(jax.random.fold_in(key, 13), 4, SEP_PIV, SEP2)


def draw_sep3_inverse(key, part):
    return draw_front(jax.random.fold_in(key, 14), 8, SEP_PIV, SEP3)


def block_scale(stream_key, extent, cuts, least, high):
    gain, own = 1.0, jax.random.fold_in(stream_key, 6)
    for axis_at, shards_of in cuts:
        draws = jnp.exp(jax.random.uniform(jax.random.fold_in(own, axis_at), (shards_of,), jnp.float32, least / len(cuts), high / len(cuts)))
        gain = gain * jnp.repeat(draws, extent[axis_at] // shards_of).reshape([-1 if axis == axis_at else 1 for axis in range(len(extent))])
    return gain


def noise(own_key, extent, spread, limit, shards=(), kind=jnp.bfloat16):
    gain = block_scale(own_key, extent, shards, -0.22, 0.18) if shards else 1.0
    drawn = jax.random.normal(own_key, extent, jnp.float32) * spread * gain
    return jnp.minimum(jnp.maximum(drawn, -limit), limit).astype(kind)


def setup_inputs(seed: int = 0) -> dict:
    streams_of = jax.random.split(jax.random.key(seed), 11)
    return {
        "app_rhs": noise(streams_of[0], (NROWS, NRHS), 1.0, 6.0, ((0, 128),), jnp.float32),
        "pivot_source": draw_pivot_source(jax.random.fold_in(streams_of[10], 71), 0),
        "row_owner": draw_row_owner(jax.random.fold_in(streams_of[10], 71), 0),
        "leaf_inverse": draw_leaf_inverse(jax.random.fold_in(streams_of[10], 71), 0),
        "leaf_coupling": noise(streams_of[4], (N_LEAF, N_FRONT, LEAF_PIV, SEP1), (0.5 * LEAF_FRONT ** -0.5), 0.054126587, ((0, 16), (1, 8)), jnp.float32),
        "sep1_inverse": draw_sep1_inverse(jax.random.fold_in(streams_of[10], 71), 0),
        "sep1_coupling": noise(streams_of[6], (N_LEAF, N_FRONT, SEP_PIV, SEP2), (0.5 * SEP1 ** -0.5), 0.06629126, ((0, 16), (1, 8)), jnp.float32),
        "sep2_inverse": draw_sep2_inverse(jax.random.fold_in(streams_of[10], 71), 0),
        "sep2_coupling": noise(streams_of[8], (N_LEAF, N_FRONT, SEP_PIV, SEP3), (0.5 * SEP2 ** -0.5), 0.046875, ((0, 16), (1, 8)), jnp.float32),
        "sep3_inverse": draw_sep3_inverse(jax.random.fold_in(streams_of[10], 71), 0),
    }


PRECISE = lax.Precision.HIGHEST


def node_form(blocked, group_size):
    leaves, fronts, pivot_rows, col_count = blocked.shape
    shaped = blocked.reshape(leaves // group_size, group_size, fronts, pivot_rows, col_count)
    shaped = jnp.transpose(shaped, (0, 2, 1, 3, 4))
    return shaped.reshape(leaves // group_size, fronts * group_size * pivot_rows, col_count)


def device_form(nodes, group_size, fronts, pivot_rows):
    node_count, row_count, col_count = nodes.shape
    shaped = nodes.reshape(node_count, fronts, group_size, pivot_rows, col_count)
    shaped = jnp.transpose(shaped, (0, 2, 1, 3, 4))
    return shaped.reshape(node_count * group_size, fronts, pivot_rows, col_count)


def apply_rows(matrices, vectors):
    return jnp.einsum("nab,nbc->nac", matrices, vectors, precision=PRECISE)


def apply_cols(matrices, vectors):
    return jnp.einsum("nba,nbc->nac", matrices, vectors, precision=PRECISE)


def pair_sum(partials):
    node_count, row_count, col_count = partials.shape
    return partials.reshape(node_count // 2, 2, row_count, col_count).sum(axis=1)


def reference(app_rhs, pivot_source, row_owner, leaf_inverse, leaf_coupling, sep1_inverse, sep1_coupling, sep2_inverse, sep2_coupling, sep3_inverse):
    leaves = leaf_inverse.shape[0]
    fronts = leaf_inverse.shape[1]
    ordered = app_rhs[pivot_source].reshape(leaves, fronts, ROWS_DEV, NRHS)
    inverses = [leaf_inverse, sep1_inverse, sep2_inverse, sep3_inverse]
    couplings = [leaf_coupling, sep1_coupling, sep2_coupling]
    pivots = [LEAF_PIV, SEP_PIV, SEP_PIV, SEP_PIV]
    starts = [0, LEAF_PIV, LEAF_PIV + SEP_PIV, LEAF_PIV + 2 * SEP_PIV]
    solved = []
    carried = None
    for height in range(4):
        group_size = 2 ** height
        own_rhs = node_form(ordered[:, :, starts[height]:starts[height] + pivots[height]], group_size)
        if height > 0:
            own_rhs = own_rhs - carried
        forward = apply_rows(node_form(inverses[height], group_size), own_rhs)
        solved.append(forward)
        if height < 3:
            carried = pair_sum(apply_cols(node_form(couplings[height], group_size), forward))
    pieces = [None, None, None, None]
    parent_sol = None
    for height in (3, 2, 1, 0):
        group_size = 2 ** height
        target = solved[height]
        if height < 3:
            target = target - apply_rows(node_form(couplings[height], group_size), jnp.repeat(parent_sol, 2, axis=0))
        parent_sol = apply_cols(node_form(inverses[height], group_size), target)
        pieces[height] = device_form(parent_sol, group_size, fronts, pivots[height])
    pivot_order = jnp.concatenate(pieces, axis=2).reshape(leaves * fronts * ROWS_DEV, NRHS)
    return pivot_order[row_owner]
```

```python
import jax
import jax.numpy as jnp
from jax import lax
from jax.sharding import PartitionSpec as P


LEAF_PIV = 384
SEP_PIV = 128
PIVOTS = (LEAF_PIV, SEP_PIV, SEP_PIV, SEP_PIV)
AXES = ("leaf", "front")
PRECISE = lax.Precision.HIGH


def same_core_groups(height):
    leaves, fronts = lax.axis_size("leaf"), lax.axis_size("front")
    span = 2**height
    return [
        [(base + leaf) * fronts + 2 * chip + core for chip in range(fronts // 2) for leaf in range(span)]
        for base in range(0, leaves, span)
        for core in range(2)
    ]


def exchange(tiles, height):
    return lax.all_to_all(
        tiles, AXES, 0, 0, axis_index_groups=same_core_groups(height), tiled=True
    )


def core_swap(block):
    count = lax.axis_size("leaf") * lax.axis_size("front")
    return lax.ppermute(block, AXES, [(i, i ^ 1) for i in range(count)])


def front_sum(partial, height):
    rows = PIVOTS[height]
    tiles = partial.reshape(-1, rows, partial.shape[1])
    return exchange(tiles, height).sum(axis=0)


def front_gather(share, height):
    count = lax.axis_size("front") // 2 * 2**height
    tiles = jnp.broadcast_to(share[None], (count, *share.shape))
    return exchange(tiles, height).reshape(-1, share.shape[1])


def core_half(matrix, core):
    rows, cols = matrix.shape
    chips = lax.axis_size("front") // 2
    slabs = matrix.reshape(rows, chips, 2, cols // (2 * chips))
    half = lax.dynamic_index_in_dim(slabs, core, 2, keepdims=False)
    return half.reshape(rows, cols // 2)


def split_matrix(matrix, core):
    return core_half(matrix, core), core_swap(core_half(matrix, 1 - core))


def both_apply(halves, vectors):
    own = jnp.dot(halves[0], vectors, precision=PRECISE)
    other = jnp.dot(halves[1], vectors, precision=PRECISE)
    there = core_swap(jnp.stack([other, own]))
    return own + there[0], other + there[1]


def both_transposed(halves, vectors):
    dims = (((0,), (0,)), ((), ()))
    return lax.dot_general(halves[0], vectors[0], dims, precision=PRECISE) + lax.dot_general(
        halves[1], vectors[1], dims, precision=PRECISE
    )


def rank_among(keys, order):
    same = (keys[:, None] == keys[None, :]) & (order[None, :] < order[:, None])
    return jnp.sum(same.astype(jnp.int32), axis=1)


def move_rows(outgoing, slot_cap):
    peers = lax.axis_size("leaf") * lax.axis_size("front")
    tiles = outgoing.reshape(peers, slot_cap, outgoing.shape[1])
    return lax.all_to_all(tiles, AXES, 0, 0, tiled=True).reshape(outgoing.shape)


def per_device(
    app_rhs,
    pivot_source,
    row_owner,
    leaf_inverse,
    leaf_coupling,
    sep1_inverse,
    sep1_coupling,
    sep2_inverse,
    sep2_coupling,
    sep3_inverse,
):
    core = lax.axis_index("front") % 2
    row_count, rhs_count = app_rhs.shape
    peers = lax.axis_size("leaf") * lax.axis_size("front")
    slot_cap = 16
    inverses = [
        split_matrix(m[0, 0], core) for m in (leaf_inverse, sep1_inverse, sep2_inverse, sep3_inverse)
    ]
    couplings = [split_matrix(m[0, 0], core) for m in (leaf_coupling, sep1_coupling, sep2_coupling)]

    destination = row_owner // row_count
    send_index = destination * slot_cap + rank_among(
        destination, jnp.arange(row_count, dtype=jnp.int32)
    )
    anchor = pivot_source // row_count
    recv_index = anchor * slot_cap + rank_among(anchor, pivot_source)
    outgoing = jnp.zeros((peers * slot_cap, rhs_count), jnp.float32).at[send_index].set(app_rhs)
    ordered = move_rows(outgoing, slot_cap)[recv_index]

    starts = (0, LEAF_PIV, LEAF_PIV + SEP_PIV, LEAF_PIV + 2 * SEP_PIV)
    solved = []
    carried = None
    for height in range(4):
        own_rhs = ordered[starts[height] : starts[height] + PIVOTS[height]]
        if height > 0:
            own_rhs = own_rhs - front_sum(carried, height)
        forward = both_apply(inverses[height], front_gather(own_rhs, height))
        solved.append(forward)
        if height < 3:
            carried = both_transposed(couplings[height], forward)
    pieces = [None, None, None, None]
    parent_sol = None
    for height in (3, 2, 1, 0):
        target = solved[height]
        if height < 3:
            update = both_apply(couplings[height], parent_sol)
            target = (target[0] - update[0], target[1] - update[1])
        share = front_sum(both_transposed(inverses[height], target), height)
        pieces[height] = share
        if height > 0:
            parent_sol = front_gather(share, height)
    pivot_order = jnp.concatenate(pieces, axis=0)
    returning = jnp.zeros((peers * slot_cap, rhs_count), jnp.float32).at[recv_index].set(pivot_order)
    return move_rows(returning, slot_cap)[send_index]


def solution(mesh):
    wide = P("leaf", "front", None, None)
    in_specs = (P(AXES, None), P(AXES), P(AXES)) + (wide,) * 7
    return jax.shard_map(
        per_device, mesh=mesh, in_specs=in_specs, out_specs=P(AXES, None), check_vma=False
    )
```

```python
import functools

import jax
import jax.numpy as jnp
from jax import lax
from jax.experimental import pallas as pl
from jax.experimental.pallas import tpu as pltpu
from jax.sharding import PartitionSpec as P


LEAF_PIV = 384
SEP_PIV = 128
PIVOTS = (LEAF_PIV, SEP_PIV, SEP_PIV, SEP_PIV)
AXES = ("leaf", "front")
F32 = jnp.float32
BF16 = jnp.bfloat16
SLOTS = 16
CHIPS = 4
VMEM = pltpu.VMEM


def params(mib=24):
    return pltpu.CompilerParams(vmem_limit_bytes=mib * 2**20)


def on_chip(x):
    return pltpu.with_memory_space_constraint(x, VMEM)


def vmem_specs(count):
    return [pl.BlockSpec(memory_space=VMEM)] * count


def call(body, outs, *args, mib=24):
    return pl.pallas_call(
        body,
        in_specs=vmem_specs(len(args)),
        out_specs=vmem_specs(len(outs)),
        out_shape=[VMEM(shape, F32) for shape in outs],
        compiler_params=params(mib),
    )(*[on_chip(a) for a in args])


def same_core_groups(height):
    leaves, fronts = lax.axis_size("leaf"), lax.axis_size("front")
    span = 2**height
    return [
        [(base + leaf) * fronts + 2 * chip + core for chip in range(fronts // 2) for leaf in range(span)]
        for base in range(0, leaves, span)
        for core in range(2)
    ]


def exchange(tiles, height):
    return lax.all_to_all(
        tiles, AXES, 0, 0, axis_index_groups=same_core_groups(height), tiled=True
    )


def core_swap(block):
    count = lax.axis_size("leaf") * lax.axis_size("front")
    return lax.ppermute(block, AXES, [(i, i ^ 1) for i in range(count)])


def pair_of(x):
    high = x.astype(BF16)
    return high, (x - high.astype(F32)).astype(BF16)


def dot(a, b):
    return jnp.dot(a, b, preferred_element_type=F32)


def send_body(core_ref, *refs):
    count = len(refs) // 2
    sources, sends, sem = refs[:count], refs[count : 2 * count], refs[-1]
    core = core_ref[0]
    copies = []
    for at in range(count):
        slab = sources[at].shape[1] // (2 * CHIPS)
        for chip in range(CHIPS):
            here = pl.ds(pl.multiple_of((2 * chip + 1 - core) * slab, 128), slab)
            copies.append(
                pltpu.make_async_copy(
                    sources[at].at[:, here],
                    sends[at].at[:, pl.ds(chip * slab, slab)],
                    sem.at[len(copies)],
                )
            )
    for copy in copies:
        copy.start()
    for copy in copies:
        copy.wait()


def sent_halves(core, matrices):
    count = len(matrices)
    out = pl.pallas_call(
        send_body,
        in_specs=[pl.BlockSpec(memory_space=pltpu.SMEM)]
        + [pl.BlockSpec(memory_space=pltpu.HBM)] * count,
        out_specs=vmem_specs(count),
        out_shape=[VMEM((m.shape[0], m.shape[1] // 2), F32) for m in matrices],
        scratch_shapes=[pltpu.SemaphoreType.DMA((CHIPS * count,))],
        compiler_params=params(4),
    )(core.reshape(1), *[pltpu.with_memory_space_constraint(m, pltpu.HBM) for m in matrices])
    return [core_swap(half) for half in out]


def matrix_specs(rows, slab):
    return [
        pl.BlockSpec((rows, slab), lambda step, core: (0, 2 * step + core[0])),
        pl.BlockSpec((rows, slab), lambda step, core: (0, step)),
    ]


def stepped(body, outs, core, matrix, other, *args, scratch=()):
    rows, slab = matrix.shape[0], other.shape[1] // CHIPS
    return pl.pallas_call(
        body,
        grid_spec=pltpu.PrefetchScalarGridSpec(
            num_scalar_prefetch=1,
            grid=(CHIPS,),
            in_specs=matrix_specs(rows, slab) + vmem_specs(len(args)),
            out_specs=vmem_specs(len(outs)),
            scratch_shapes=list(scratch),
        ),
        out_shape=[VMEM(shape, F32) for shape in outs],
        compiler_params=params(16),
    )(core.reshape(1), matrix, other, *[on_chip(a) for a in args])


def apply_body(core_ref, own_ref, other_ref, vec_ref, out_ref, acc_ref):
    rows, slab = own_ref.shape
    both, width = 2 * rows, vec_ref.shape[1]
    step = pl.program_id(0)
    at = pl.ds(pl.multiple_of(step * slab, 128), slab)
    left = pair_of(jnp.concatenate([own_ref[...], other_ref[...]], axis=0))
    right = pair_of(vec_ref[at, :])
    full = dot(jnp.concatenate(left, axis=0), jnp.concatenate(right, axis=1))
    total = full[:both, :width] + full[:both, width:]
    total += full[both:, :width] + full[both:, width:]

    @pl.when(step == 0)
    def _():
        acc_ref[...] = total

    @pl.when(step > 0)
    def _():
        acc_ref[...] += total

    @pl.when(step == CHIPS - 1)
    def _():
        out_ref[0] = acc_ref[rows:]
        out_ref[1] = acc_ref[:rows]


def both_apply(core, matrix, other, vectors):
    rows, width = matrix.shape[0], vectors.shape[1]
    (out,) = stepped(
        apply_body,
        [(2, rows, width)],
        core,
        matrix,
        other,
        vectors,
        scratch=[VMEM((2 * rows, width), F32)],
    )
    return out


def spread(own_ref, other_ref, vector, out_ref):
    high, low = pair_of(vector.T)
    left = jnp.concatenate([high, low], axis=0)
    width, slab = vector.shape[1], own_ref.shape[1]
    at = pl.ds(pl.multiple_of(pl.program_id(0) * slab, 128), slab)
    up, down = pair_of(jnp.concatenate([own_ref[...], other_ref[...]], axis=0))
    full = dot(left, up) + dot(left, down)
    out_ref[at, :] = (full[:width] + full[width:]).T


def joined(here_ref, there_ref):
    return jnp.concatenate([here_ref[1] + there_ref[0], here_ref[0] + there_ref[1]], axis=0)


def forward_body(core_ref, own_ref, other_ref, here_ref, there_ref, out_ref, solved_ref):
    solved = joined(here_ref, there_ref)
    solved_ref[...] = solved
    spread(own_ref, other_ref, solved, out_ref)


def top_body(core_ref, own_ref, other_ref, here_ref, there_ref, out_ref):
    spread(own_ref, other_ref, joined(here_ref, there_ref), out_ref)


def backward_body(core_ref, own_ref, other_ref, here_ref, there_ref, solved_ref, out_ref):
    spread(own_ref, other_ref, solved_ref[...] - joined(here_ref, there_ref), out_ref)


def minus_sum_body(tiles_ref, base_ref, out_ref):
    share = base_ref[...] - jnp.sum(tiles_ref[...], axis=0)
    out_ref[...] = jnp.broadcast_to(share[None], out_ref.shape)


def sum_body(tiles_ref, share_ref, out_ref):
    share = jnp.sum(tiles_ref[...], axis=0)
    share_ref[...] = share
    out_ref[...] = jnp.broadcast_to(share[None], out_ref.shape)


def slots_body(index_ref, rows_ref, out_ref):
    rows = rows_ref[...]
    width = rows.shape[1]
    high, rest = pair_of(rows)
    middle = rest
    low = (rows - high.astype(F32) - middle.astype(F32)).astype(BF16)
    parts = jnp.concatenate([high, middle, low], axis=1)
    index = index_ref[...]

    @pl.loop(0, out_ref.shape[0] // 256)
    def _(step):
        start = pl.multiple_of(step * 256, 256)
        slot = lax.broadcasted_iota(jnp.int32, (256, rows.shape[0]), 0) + start
        chosen = dot((slot == index).astype(F32).astype(BF16), parts)
        out_ref[pl.ds(start, 256), :] = (
            chosen[:, :width] + chosen[:, width : 2 * width] + chosen[:, 2 * width :]
        )


def to_slots(index, rows):
    peers = lax.axis_size("leaf") * lax.axis_size("front")
    return pl.pallas_call(
        slots_body,
        in_specs=vmem_specs(2),
        out_specs=pl.BlockSpec(memory_space=VMEM),
        out_shape=VMEM((peers * SLOTS, rows.shape[1]), F32),
        compiler_params=params(),
    )(index[None, :], rows)


def rank_among(keys, order):
    same = (keys[:, None] == keys[None, :]) & (order[None, :] < order[:, None])
    return jnp.sum(same.astype(jnp.int32), axis=1)


def move_rows(outgoing):
    tiles = outgoing.reshape(-1, SLOTS, outgoing.shape[1])
    return lax.all_to_all(tiles, AXES, 0, 0, tiled=True).reshape(outgoing.shape)


def per_device(app_rhs, pivot_source, row_owner, *matrices):
    core = lax.axis_index("front") % 2
    row_count, width = app_rhs.shape
    matrices = [m[0, 0] for m in matrices]
    halves = list(zip(matrices, sent_halves(core, matrices)))
    inverses = (halves[0], halves[2], halves[4], halves[6])
    couplings = (halves[1], halves[3], halves[5])

    destination = row_owner // row_count
    send_index = destination * SLOTS + rank_among(
        destination, jnp.arange(row_count, dtype=jnp.int32)
    )
    anchor = pivot_source // row_count
    recv_index = anchor * SLOTS + rank_among(anchor, pivot_source)
    ordered = move_rows(to_slots(send_index, app_rhs))[recv_index]

    starts = (0, LEAF_PIV, LEAF_PIV + SEP_PIV, LEAF_PIV + 2 * SEP_PIV)
    sizes = [CHIPS * 2**height for height in range(4)]
    own = [ordered[at : at + rows] for at, rows in zip(starts, PIVOTS)]
    tiles = jnp.broadcast_to(own[0][None], (sizes[0], LEAF_PIV, width))
    solved = []
    for height in range(4):
        gathered = exchange(tiles, height).reshape(-1, width)
        here = both_apply(core, *inverses[height], gathered)
        there = core_swap(here)
        if height == 3:
            break
        mats = couplings[height]
        outs = [(mats[1].shape[1], width), (2 * PIVOTS[height], width)]
        carried, forward = stepped(forward_body, outs, core, *mats, here, there)
        solved.append(forward)
        arrived = exchange(carried.reshape(-1, SEP_PIV, width), height + 1)
        (tiles,) = call(
            minus_sum_body, [(sizes[height + 1], SEP_PIV, width)], arrived, own[height + 1]
        )
    (spread_out,) = stepped(
        top_body, [(inverses[3][1].shape[1], width)], core, *inverses[3], here, there
    )
    pieces = [None, None, None, None]
    for height in (3, 2, 1):
        arrived = exchange(spread_out.reshape(-1, SEP_PIV, width), height)
        pieces[height], tiles = call(
            sum_body, [(SEP_PIV, width), (sizes[height], SEP_PIV, width)], arrived
        )
        parent = exchange(tiles, height).reshape(-1, width)
        here = both_apply(core, *couplings[height - 1], parent)
        there = core_swap(here)
        mats = inverses[height - 1]
        outs = [(mats[1].shape[1], width)]
        (spread_out,) = stepped(backward_body, outs, core, *mats, here, there, solved[height - 1])
    pieces[0] = exchange(spread_out.reshape(-1, LEAF_PIV, width), 0).sum(axis=0)
    pivot_order = jnp.concatenate(pieces, axis=0)
    return move_rows(to_slots(recv_index, pivot_order))[send_index]


def solution(mesh):
    wide = P("leaf", "front", None, None)
    in_specs = (P(AXES, None), P(AXES), P(AXES)) + (wide,) * 7
    return jax.shard_map(
        per_device, mesh=mesh, in_specs=in_specs, out_specs=P(AXES, None), check_vma=False
    )
```

```python
import jax
import jax.numpy as jnp
from jax import lax
from jax.experimental import pallas as pl
from jax.experimental.pallas import tpu as pltpu
from jax.sharding import PartitionSpec as P


LEAF_PIV = 384
SEP_PIV = 128
PIVOTS = (LEAF_PIV, SEP_PIV, SEP_PIV, SEP_PIV)
AXES = ("leaf", "front")
F32 = jnp.float32
BF16 = jnp.bfloat16
SLOTS = 16
CHIPS = 4
CORE = 1
PLANE = 32
VMEM = pltpu.VMEM
HBM = pltpu.HBM


def params(mib):
    return pltpu.CompilerParams(vmem_limit_bytes=mib * 2**20)


def on_chip(x):
    return pltpu.with_memory_space_constraint(x, VMEM)


def off_chip(x):
    return pltpu.with_memory_space_constraint(x, HBM)


def vmem_specs(count):
    return [pl.BlockSpec(memory_space=VMEM)] * count


def call(body, outs, *args):
    return pl.pallas_call(
        body,
        in_specs=vmem_specs(len(args)),
        out_specs=vmem_specs(len(outs)),
        out_shape=[VMEM(shape, F32) for shape in outs],
        compiler_params=params(16),
    )(*[on_chip(a) for a in args])


def same_core_groups(height):
    leaves, fronts = lax.axis_size("leaf"), lax.axis_size("front")
    span = 2**height
    return [
        [(base + leaf) * fronts + 2 * chip + core for chip in range(fronts // 2) for leaf in range(span)]
        for base in range(0, leaves, span)
        for core in range(2)
    ]


def exchange(tiles, height):
    return lax.all_to_all(
        tiles, AXES, 0, 0, axis_index_groups=same_core_groups(min(height, 2)), tiled=True
    )


def swap(block, mask):
    count = lax.axis_size("leaf") * lax.axis_size("front")
    return lax.ppermute(block, AXES, [(i, i ^ mask) for i in range(count)])


def pair_of(x):
    high = x.astype(BF16)
    return high, (x - high.astype(F32)).astype(BF16)


def dot(a, b):
    return jnp.dot(a, b, preferred_element_type=F32)


def send_body(pieces, at_ref, *refs):
    count = len(pieces)
    sources = refs[: pieces[-1][0] + 1]
    sends = refs[len(sources) : len(sources) + count]
    stages = refs[len(sources) + count : len(sources) + 2 * count]
    in_sem, out_sem = refs[-2:]
    inward, outward = [], []
    for number, (source, cuts, place) in enumerate(pieces):
        width = stages[number].shape[1] // CHIPS
        inward.append([])
        for chip in range(CHIPS):
            block = 2 * cuts * chip + at_ref[place]
            here = pl.ds(pl.multiple_of(block * width, 128), width)
            inward[-1].append(
                pltpu.make_async_copy(
                    sources[source].at[:, here],
                    stages[number].at[:, pl.ds(chip * width, width)],
                    in_sem.at[number * CHIPS + chip],
                )
            )
        outward.append(pltpu.make_async_copy(stages[number], sends[number], out_sem.at[number]))
    for group in inward:
        for copy in group:
            copy.start()
    for group, after in zip(inward, outward):
        for copy in group:
            copy.wait()
        after.start()
    for copy in outward:
        copy.wait()


def cut_sends(places, matrices, pieces):
    shapes = [(matrices[m].shape[0], matrices[m].shape[1] // (2 * cuts)) for m, cuts, _ in pieces]
    return pl.pallas_call(
        lambda *refs: send_body(pieces, *refs),
        in_specs=[pl.BlockSpec(memory_space=pltpu.SMEM)]
        + [pl.BlockSpec(memory_space=HBM)] * len(matrices),
        out_specs=[pl.BlockSpec(memory_space=HBM)] * len(pieces),
        out_shape=[HBM(shape, F32) for shape in shapes],
        scratch_shapes=[VMEM(shape, F32) for shape in shapes]
        + [
            pltpu.SemaphoreType.DMA((CHIPS * len(pieces),)),
            pltpu.SemaphoreType.DMA((len(pieces),)),
        ],
        compiler_params=params(20),
    )(places, *[off_chip(m) for m in matrices])


def stepped(body, outs, places, mats, *args, scratch=()):
    matrix, others = mats[0], mats[1:]
    rows, width = others[0].shape[0], others[0].shape[1] // CHIPS
    cuts = matrix.shape[1] // (2 * CHIPS * width)
    own = pl.BlockSpec((rows, width), lambda step, at: (0, 2 * cuts * step + at[cuts - 1]))
    rest = pl.BlockSpec((rows, width), lambda step, at: (0, step))
    return pl.pallas_call(
        body,
        grid_spec=pltpu.PrefetchScalarGridSpec(
            num_scalar_prefetch=1,
            grid=(CHIPS,),
            in_specs=[own] + [rest] * len(others) + vmem_specs(len(args)),
            out_specs=vmem_specs(len(outs)),
            scratch_shapes=list(scratch),
        ),
        out_shape=[VMEM(shape, F32) for shape in outs],
        compiler_params=params(16),
    )(places, off_chip(matrix), *[off_chip(m) for m in others], *[on_chip(a) for a in args])


def apply_body(at_ref, *refs):
    blocks, (vec_ref, out_ref, acc_ref) = refs[:-3], refs[-3:]
    rows, width = blocks[0].shape
    total_rows, count = len(blocks) * rows, vec_ref.shape[1]
    step = pl.program_id(0)
    at = pl.ds(pl.multiple_of(step * width, 128), width)
    left = pair_of(jnp.concatenate([b[...] for b in blocks], axis=0))
    right = pair_of(vec_ref[at, :])
    full = dot(jnp.concatenate(left, axis=0), jnp.concatenate(right, axis=1))
    total = full[:total_rows, :count] + full[:total_rows, count:]
    total += full[total_rows:, :count] + full[total_rows:, count:]

    @pl.when(step == 0)
    def _():
        acc_ref[...] = total

    @pl.when(step > 0)
    def _():
        acc_ref[...] += total

    @pl.when(step == CHIPS - 1)
    def _():
        for part in range(len(blocks)):
            out_ref[part] = acc_ref[part * rows : (part + 1) * rows]


def applied(places, mats, vectors):
    rows, count = mats[0].shape[0], vectors.shape[1]
    shape = (len(mats), rows, count)
    acc = VMEM((len(mats) * rows, count), F32)
    (out,) = stepped(apply_body, [shape], places, mats, vectors, scratch=[acc])
    return out


def spread(blocks, vector, out_ref):
    high, low = pair_of(vector.T)
    left = jnp.concatenate([high, low], axis=0)
    count, width = vector.shape[1], blocks[0].shape[1]
    at = pl.ds(pl.multiple_of(pl.program_id(0) * width, 128), width)
    up, down = pair_of(jnp.concatenate([b[...] for b in blocks], axis=0))
    full = dot(left, up) + dot(left, down)
    out_ref[at, :] = (full[:count] + full[count:]).T


def rows_of(*tiles):
    return jnp.concatenate(tiles, axis=0)


def joined(here_ref, there_ref):
    return rows_of(here_ref[0] + there_ref[1], here_ref[1] + there_ref[0])


def forward_body(at_ref, *refs):
    blocks, (here_ref, there_ref, out_ref, solved_ref) = refs[:-4], refs[-4:]
    solved = joined(here_ref, there_ref)
    solved_ref[...] = solved
    spread(blocks, solved, out_ref)


def plane_body(at_ref, *refs):
    blocks, (solved_ref, far_ref, out_ref) = refs[:-3], refs[-3:]
    spread(blocks, rows_of(solved_ref[...], far_ref[...]), out_ref)


def top_body(at_ref, *refs):
    blocks, (here_ref, there_ref, out_ref) = refs[:-3], refs[-3:]
    vector = rows_of(*[here_ref[part] + there_ref[part ^ 2] for part in range(4)])
    spread(blocks, vector, out_ref)


def backward_body(at_ref, *refs):
    blocks, (here_ref, there_ref, solved_ref, out_ref) = refs[:-4], refs[-4:]
    spread(blocks, solved_ref[...] - joined(here_ref, there_ref), out_ref)


def joined_body(here_ref, there_ref, out_ref):
    out_ref[...] = joined(here_ref, there_ref)


def core_pair_body(here_ref, there_ref, out_ref):
    for part in range(4):
        out_ref[part] = here_ref[part] + there_ref[part ^ 1]


def plane_pair_body(here_ref, there_ref, out_ref):
    for part in range(2):
        out_ref[part] = here_ref[part] + there_ref[part]


def minus_sum_body(tiles_ref, base_ref, out_ref):
    share = base_ref[...] - jnp.sum(tiles_ref[...], axis=0)
    out_ref[...] = jnp.broadcast_to(share[None], out_ref.shape)


def sum_body(tiles_ref, share_ref, out_ref):
    share = jnp.sum(tiles_ref[...], axis=0)
    share_ref[...] = share
    out_ref[...] = jnp.broadcast_to(share[None], out_ref.shape)


def slots_body(index_ref, rows_ref, out_ref):
    rows = rows_ref[...]
    width = rows.shape[1]
    high, middle = pair_of(rows)
    low = (rows - high.astype(F32) - middle.astype(F32)).astype(BF16)
    parts = jnp.concatenate([high, middle, low], axis=1)
    index = index_ref[...]

    @pl.loop(0, out_ref.shape[0] // 256)
    def _(step):
        start = pl.multiple_of(step * 256, 256)
        slot = lax.broadcasted_iota(jnp.int32, (256, rows.shape[0]), 0) + start
        chosen = dot((slot == index).astype(F32).astype(BF16), parts)
        out_ref[pl.ds(start, 256), :] = (
            chosen[:, :width] + chosen[:, width : 2 * width] + chosen[:, 2 * width :]
        )


def to_slots(index, rows):
    peers = lax.axis_size("leaf") * lax.axis_size("front")
    return pl.pallas_call(
        slots_body,
        in_specs=vmem_specs(2),
        out_specs=pl.BlockSpec(memory_space=VMEM),
        out_shape=VMEM((peers * SLOTS, rows.shape[1]), F32),
        compiler_params=params(16),
    )(index[None, :], rows)


def rank_among(keys, order):
    same = (keys[:, None] == keys[None, :]) & (order[None, :] < order[:, None])
    return jnp.sum(same.astype(jnp.int32), axis=1)


def move_rows(outgoing):
    tiles = outgoing.reshape(-1, SLOTS, outgoing.shape[1])
    return lax.all_to_all(tiles, AXES, 0, 0, tiled=True).reshape(outgoing.shape)


def whole_solve(app_rhs, pivot_source, row_owner, *matrices):
    core = lax.axis_index("front") % 2
    plane = lax.axis_index("leaf") // 4 % 2
    row_count, width = app_rhs.shape
    matrices = [m[0, 0] for m in matrices]

    destination = row_owner // row_count
    send_index = destination * SLOTS + rank_among(
        destination, jnp.arange(row_count, dtype=jnp.int32)
    )
    anchor = pivot_source // row_count
    recv_index = anchor * SLOTS + rank_among(anchor, pivot_source)
    outgoing = to_slots(send_index, app_rhs)

    def all_places(core, plane):
        near, far = 2 * core + plane, 2 * (1 - core) + plane
        table = [core, near, 1 - core, far, near + 1 - 2 * plane, far + 1 - 2 * plane]
        return jnp.stack(table).astype(jnp.int32)

    places = all_places(core, plane)
    sends = cut_sends(places, matrices[:2], [(0, 1, 2), (1, 1, 2)])
    mats = [[matrices[m], swap(sends[m], CORE)] for m in range(2)]
    ordered = move_rows(outgoing)[recv_index]
    ordered, core, plane = lax.optimization_barrier((ordered, core, plane))
    late = [(m, 1, 2) for m in range(3)] + [(m, 2, p) for m in (3, 4) for p in (3, 4, 5)]
    sends = cut_sends(all_places(core, plane), matrices[2:], late)
    mats += [[matrices[m], swap(sends[m - 2], CORE)] for m in range(2, 5)]
    mats += [[matrices[m], swap(sends[3 * m - 12], CORE)] for m in (5, 6)]
    for number, piece in enumerate((4, 5, 7, 8)):
        half = swap(sends[piece], (PLANE, PLANE | CORE)[number % 2])
        mats[5 + number // 2].append(half)
    inverses = (mats[0], mats[2], mats[4], mats[6])
    couplings = (mats[1], mats[3], mats[5])

    starts = (0, LEAF_PIV, LEAF_PIV + SEP_PIV, LEAF_PIV + 2 * SEP_PIV)
    sizes = (CHIPS, 2 * CHIPS, 4 * CHIPS, 4 * CHIPS)
    own = [ordered[at : at + rows] for at, rows in zip(starts, PIVOTS)]
    tiles = jnp.broadcast_to(own[0][None], (sizes[0], LEAF_PIV, width))
    solved = []
    for height in range(3):
        gathered = exchange(tiles, height).reshape(-1, width)
        here = applied(places, inverses[height], gathered)
        there = swap(here, CORE)
        outs = [(couplings[height][1].shape[1], width), (2 * PIVOTS[height], width)]
        if height < 2:
            carried, forward = stepped(
                forward_body, outs, places, couplings[height], here, there
            )
        else:
            (forward,) = call(joined_body, outs[1:], here, there)
            far_rows = swap(forward, PLANE)
            (carried,) = stepped(
                plane_body, outs[:1], places, couplings[height], forward, far_rows
            )
        solved.append(forward)
        arrived = exchange(carried.reshape(-1, SEP_PIV, width), height + 1)
        (tiles,) = call(
            minus_sum_body, [(sizes[height + 1], SEP_PIV, width)], arrived, own[height + 1]
        )
    here = applied(places, inverses[3], exchange(tiles, 3).reshape(-1, width))
    (here,) = call(core_pair_body, [here.shape], here, swap(here, CORE))
    (spread_out,) = stepped(
        top_body, [(inverses[3][1].shape[1], width)], places, inverses[3], here, swap(here, PLANE)
    )
    pieces = [None, None, None, None]
    for height in (3, 2, 1):
        arrived = exchange(spread_out.reshape(-1, SEP_PIV, width), height)
        pieces[height], tiles = call(
            sum_body, [(SEP_PIV, width), (sizes[height], SEP_PIV, width)], arrived
        )
        here = applied(places, couplings[height - 1], exchange(tiles, height).reshape(-1, width))
        if height == 3:
            (here,) = call(plane_pair_body, [(2, SEP_PIV, width)], here, swap(here[2:], PLANE))
        there = swap(here, CORE)
        mats_low = inverses[height - 1]
        outs = [(mats_low[1].shape[1], width)]
        (spread_out,) = stepped(
            backward_body, outs, places, mats_low, here, there, solved[height - 1]
        )
    pieces[0] = exchange(spread_out.reshape(-1, LEAF_PIV, width), 0).sum(axis=0)
    pivot_order = jnp.concatenate(pieces, axis=0)
    return move_rows(to_slots(recv_index, pivot_order))[send_index]


def solution(mesh):
    wide = P("leaf", "front", None, None)
    in_specs = (P(AXES, None), P(AXES), P(AXES)) + (wide,) * 7
    return jax.shard_map(
        whole_solve, mesh=mesh, in_specs=in_specs, out_specs=P(AXES, None), check_vma=False
    )
```

```python
import jax
import jax.numpy as jnp
from jax import lax
from jax.experimental import pallas as pl
from jax.experimental.pallas import tpu as pltpu
from jax.sharding import PartitionSpec as P


LEAF_PIV = 384
SEP_PIV = 128
PIVOTS = (LEAF_PIV, SEP_PIV, SEP_PIV, SEP_PIV)
AXES = ("leaf", "front")
F32 = jnp.float32
BF16 = jnp.bfloat16
SLOTS = 16
CHIPS = 4
CORE = 1
PLANE = 32
VMEM = pltpu.VMEM
HBM = pltpu.HBM


def params(mib):
    return pltpu.CompilerParams(vmem_limit_bytes=mib * 2**20)


def on_chip(x):
    return pltpu.with_memory_space_constraint(x, VMEM)


def off_chip(x):
    return pltpu.with_memory_space_constraint(x, HBM)


def vmem_specs(count):
    return [pl.BlockSpec(memory_space=VMEM)] * count


def call(body, outs, *args):
    return pl.pallas_call(
        body,
        in_specs=vmem_specs(len(args)),
        out_specs=vmem_specs(len(outs)),
        out_shape=[VMEM(shape, F32) for shape in outs],
        compiler_params=params(16),
    )(*[on_chip(a) for a in args])


def same_core_groups(height):
    leaves, fronts = lax.axis_size("leaf"), lax.axis_size("front")
    span = 2**height
    return [
        [(base + leaf) * fronts + 2 * chip + core for chip in range(fronts // 2) for leaf in range(span)]
        for base in range(0, leaves, span)
        for core in range(2)
    ]


def exchange(tiles, height):
    return lax.all_to_all(
        tiles, AXES, 0, 0, axis_index_groups=same_core_groups(min(height, 2)), tiled=True
    )


def swap(block, mask):
    count = lax.axis_size("leaf") * lax.axis_size("front")
    return lax.ppermute(block, AXES, [(i, i ^ mask) for i in range(count)])


def pair_of(x):
    high = x.astype(BF16)
    return high, (x - high.astype(F32)).astype(BF16)


def dot(a, b):
    return jnp.dot(a, b, preferred_element_type=F32)


def moves(pieces, at_ref, sources, sends, stages, in_sem, out_sem):
    inward, outward = [], []
    for number, (source, cuts, place) in enumerate(pieces):
        width = stages[number].shape[1] // CHIPS
        inward.append([])
        for chip in range(CHIPS):
            block = 2 * cuts * chip + at_ref[place]
            here = pl.ds(pl.multiple_of(block * width, 128), width)
            inward[-1].append(
                pltpu.make_async_copy(
                    sources[source].at[:, here],
                    stages[number].at[:, pl.ds(chip * width, width)],
                    in_sem.at[number * CHIPS + chip],
                )
            )
        outward.append(pltpu.make_async_copy(stages[number], sends[number], out_sem.at[number]))
    return inward, outward


def cut_sends(places, matrices, pieces, index=None, rows=None):
    shapes = [(matrices[m].shape[0], matrices[m].shape[1] // (2 * cuts)) for m, cuts, _ in pieces]
    count, total = len(pieces), len(matrices)
    extra = [] if rows is None else [index[None, :], rows]

    def body(at_ref, *refs):
        sources, refs = refs[:total], refs[total:]
        given, refs = refs[: len(extra)], refs[len(extra) :]
        sends, refs = refs[:count], refs[count:]
        filled, refs = refs[: len(extra) // 2], refs[len(extra) // 2 :]
        stages, sems = refs[:count], refs[count:]
        inward, outward = moves(pieces, at_ref, sources, sends, stages, *sems)
        for group in inward:
            for copy in group:
                copy.start()
        if extra:
            slots_body(*given, *filled)
        for group, after in zip(inward, outward):
            for copy in group:
                copy.wait()
            after.start()
        for copy in outward:
            copy.wait()

    peers = lax.axis_size("leaf") * lax.axis_size("front")
    slots = [] if rows is None else [VMEM((peers * SLOTS, rows.shape[1]), F32)]
    return pl.pallas_call(
        body,
        in_specs=[pl.BlockSpec(memory_space=pltpu.SMEM)]
        + [pl.BlockSpec(memory_space=HBM)] * total
        + vmem_specs(len(extra)),
        out_specs=[pl.BlockSpec(memory_space=HBM)] * count + vmem_specs(len(slots)),
        out_shape=[HBM(shape, F32) for shape in shapes] + slots,
        scratch_shapes=[VMEM(shape, F32) for shape in shapes]
        + [pltpu.SemaphoreType.DMA((CHIPS * count,)), pltpu.SemaphoreType.DMA((count,))],
        compiler_params=params(20),
    )(places, *[off_chip(m) for m in matrices], *extra)


def shape_of(mats):
    return (len(mats) * mats[1].shape[0], mats[1].shape[1])


def loads(at_ref, sources, held, sem):
    parts = len(sources)
    rows, width = held.shape[0] // parts, held.shape[1] // CHIPS
    cuts = sources[0].shape[1] // (2 * CHIPS * width)

    def copy(part, step):
        there = pl.ds(pl.multiple_of(step * width, 128), width)
        block = 2 * cuts * step + at_ref[cuts - 1] if part == 0 else step
        here = pl.ds(pl.multiple_of(block * width, 128), width)
        return pltpu.make_async_copy(
            sources[part].at[:, here], held.at[pl.ds(part * rows, rows), there], sem.at[part, step]
        )

    def start():
        for step in range(CHIPS):
            for part in range(parts):
                copy(part, step).start()

    def wait(step):
        for part in range(parts):
            copy(part, step).wait()

    return start, wait


def applied(places, mats, vectors, following=None):
    parts, rows, count = len(mats), mats[1].shape[0], vectors.shape[1]
    extra = list(following or [])

    def body(at_ref, *refs):
        sources, later = refs[:parts], refs[parts : parts + len(extra)]
        vec_ref, out_ref, kept_ref = refs[parts + len(extra) : parts + len(extra) + 3]
        acc_ref, sem, late_sem, *spare = refs[parts + len(extra) + 3 :]
        held = spare[0] if extra else kept_ref
        start, wait = loads(at_ref, sources, held, sem)
        start()
        if extra:
            late_start, late_wait = loads(at_ref, later, kept_ref, late_sem)
            late_start()
        width = held.shape[1] // CHIPS
        acc_ref[...] = jnp.zeros(acc_ref.shape, F32)

        @pl.loop(0, CHIPS)
        def _(step):
            wait(step)
            at = pl.ds(pl.multiple_of(step * width, 128), width)
            high, low = pair_of(held[:, at])
            right = jnp.concatenate(pair_of(vec_ref[at, :]), axis=1)
            full = dot(high, right) + dot(low, right)
            acc_ref[...] += full[:, :count] + full[:, count:]

        for part in range(parts):
            out_ref[part] = acc_ref[part * rows : (part + 1) * rows]
        if extra:
            for step in range(CHIPS):
                late_wait(step)

    kept = shape_of(extra or mats)
    return pl.pallas_call(
        body,
        in_specs=[pl.BlockSpec(memory_space=pltpu.SMEM)]
        + [pl.BlockSpec(memory_space=HBM)] * (parts + len(extra))
        + vmem_specs(1),
        out_specs=vmem_specs(2),
        out_shape=[VMEM((parts, rows, count), F32), VMEM(kept, F32)],
        scratch_shapes=[
            VMEM((parts * rows, count), F32),
            pltpu.SemaphoreType.DMA((parts, CHIPS)),
            pltpu.SemaphoreType.DMA((max(1, len(extra)), CHIPS)),
        ]
        + ([VMEM(shape_of(mats), F32)] if extra else []),
        compiler_params=params(20),
    )(places, *[off_chip(m) for m in list(mats) + extra], on_chip(vectors))


def spread(held_ref, vector, out_ref):
    left = jnp.concatenate(pair_of(vector.T), axis=0)
    count, width = vector.shape[1], held_ref.shape[1] // CHIPS

    @pl.loop(0, CHIPS)
    def _(step):
        at = pl.ds(pl.multiple_of(step * width, 128), width)
        up, down = pair_of(held_ref[:, at])
        full = dot(left, up) + dot(left, down)
        out_ref[at, :] = (full[:count] + full[count:]).T


def rows_of(*tiles):
    return jnp.concatenate(tiles, axis=0)


def joined(here_ref, there_ref):
    return rows_of(here_ref[0] + there_ref[1], here_ref[1] + there_ref[0])


def forward_body(held_ref, here_ref, there_ref, out_ref, solved_ref):
    solved = joined(here_ref, there_ref)
    solved_ref[...] = solved
    spread(held_ref, solved, out_ref)


def plane_body(held_ref, solved_ref, far_ref, out_ref):
    spread(held_ref, rows_of(solved_ref[...], far_ref[...]), out_ref)


def top_body(held_ref, here_ref, there_ref, out_ref):
    vector = rows_of(*[here_ref[part] + there_ref[part ^ 2] for part in range(4)])
    spread(held_ref, vector, out_ref)


def backward_body(held_ref, here_ref, there_ref, solved_ref, out_ref):
    spread(held_ref, solved_ref[...] - joined(here_ref, there_ref), out_ref)


def joined_body(here_ref, there_ref, out_ref):
    out_ref[...] = joined(here_ref, there_ref)


def core_pair_body(here_ref, there_ref, out_ref):
    for part in range(4):
        out_ref[part] = here_ref[part] + there_ref[part ^ 1]


def plane_pair_body(here_ref, there_ref, out_ref):
    for part in range(2):
        out_ref[part] = here_ref[part] + there_ref[part]


def minus_sum_body(tiles_ref, base_ref, out_ref):
    share = base_ref[...] - jnp.sum(tiles_ref[...], axis=0)
    out_ref[...] = jnp.broadcast_to(share[None], out_ref.shape)


def sum_body(tiles_ref, share_ref, out_ref):
    share = jnp.sum(tiles_ref[...], axis=0)
    share_ref[...] = share
    out_ref[...] = jnp.broadcast_to(share[None], out_ref.shape)


def slots_body(index_ref, rows_ref, out_ref):
    parts = jnp.concatenate(pair_of(rows_ref[...]), axis=1)
    count, width = rows_ref.shape
    index = index_ref[...]

    @pl.loop(0, out_ref.shape[0] // 512)
    def _(step):
        start = pl.multiple_of(step * 512, 512)
        slot = lax.broadcasted_iota(jnp.int32, (512, count), 0) + start
        chosen = dot((slot == index).astype(F32).astype(BF16), parts)
        out_ref[pl.ds(start, 512), :] = chosen[:, :width] + chosen[:, width:]


def to_slots(index, rows):
    peers = lax.axis_size("leaf") * lax.axis_size("front")
    return pl.pallas_call(
        slots_body,
        in_specs=vmem_specs(2),
        out_specs=pl.BlockSpec(memory_space=VMEM),
        out_shape=VMEM((peers * SLOTS, rows.shape[1]), F32),
        compiler_params=params(16),
    )(index[None, :], rows)


def rank_among(keys, order):
    same = (keys[:, None] == keys[None, :]) & (order[None, :] < order[:, None])
    return jnp.sum(same.astype(jnp.int32), axis=1)


def move_rows(outgoing):
    tiles = outgoing.reshape(-1, SLOTS, outgoing.shape[1])
    return lax.all_to_all(tiles, AXES, 0, 0, tiled=True).reshape(outgoing.shape)


def whole_solve(app_rhs, pivot_source, row_owner, *matrices):
    core = lax.axis_index("front") % 2
    plane = lax.axis_index("leaf") // 4 % 2
    row_count, width = app_rhs.shape
    matrices = [m[0, 0] for m in matrices]

    destination = row_owner // row_count
    send_index = destination * SLOTS + rank_among(
        destination, jnp.arange(row_count, dtype=jnp.int32)
    )
    anchor = pivot_source // row_count
    recv_index = anchor * SLOTS + rank_among(anchor, pivot_source)

    def all_places(core, plane):
        near, far = 2 * core + plane, 2 * (1 - core) + plane
        table = [core, near, 1 - core, far, near + 1 - 2 * plane, far + 1 - 2 * plane]
        return jnp.stack(table).astype(jnp.int32)

    places = all_places(core, plane)
    first = [(0, 1, 2), (1, 1, 2)]
    *sends, outgoing = cut_sends(places, matrices[:2], first, send_index, app_rhs)
    mats = [[matrices[m], swap(sends[m], CORE)] for m in range(2)]
    ordered = move_rows(outgoing)[recv_index]
    ordered, core, plane = lax.optimization_barrier((ordered, core, plane))
    late = [(m, 1, 2) for m in range(3)] + [(m, 2, p) for m in (3, 4) for p in (3, 4, 5)]
    sends = cut_sends(all_places(core, plane), matrices[2:], late)
    mats += [[matrices[m], swap(sends[m - 2], CORE)] for m in range(2, 5)]
    mats += [[matrices[m], swap(sends[3 * m - 12], CORE)] for m in (5, 6)]
    for number, piece in enumerate((4, 5, 7, 8)):
        half = swap(sends[piece], (PLANE, PLANE | CORE)[number % 2])
        mats[5 + number // 2].append(half)
    inverses = (mats[0], mats[2], mats[4], mats[6])
    couplings = (mats[1], mats[3], mats[5])

    starts = (0, LEAF_PIV, LEAF_PIV + SEP_PIV, LEAF_PIV + 2 * SEP_PIV)
    sizes = (CHIPS, 2 * CHIPS, 4 * CHIPS, 4 * CHIPS)
    own = [ordered[at : at + rows] for at, rows in zip(starts, PIVOTS)]
    tiles = jnp.broadcast_to(own[0][None], (sizes[0], LEAF_PIV, width))
    solved = []
    for height in range(3):
        gathered = exchange(tiles, height).reshape(-1, width)
        here, held = applied(places, inverses[height], gathered, couplings[height])
        there = swap(here, CORE)
        outs = [(held.shape[1], width), (2 * PIVOTS[height], width)]
        if height < 2:
            carried, forward = call(forward_body, outs, held, here, there)
        else:
            (forward,) = call(joined_body, outs[1:], here, there)
            (carried,) = call(plane_body, outs[:1], held, forward, swap(forward, PLANE))
        solved.append(forward)
        arrived = exchange(carried.reshape(-1, SEP_PIV, width), height + 1)
        (tiles,) = call(
            minus_sum_body, [(sizes[height + 1], SEP_PIV, width)], arrived, own[height + 1]
        )
    here, held = applied(places, inverses[3], exchange(tiles, 3).reshape(-1, width))
    (here,) = call(core_pair_body, [here.shape], here, swap(here, CORE))
    (spread_out,) = call(top_body, [(held.shape[1], width)], held, here, swap(here, PLANE))
    pieces = [None, None, None, None]
    for height in (3, 2, 1):
        arrived = exchange(spread_out.reshape(-1, SEP_PIV, width), height)
        pieces[height], tiles = call(
            sum_body, [(SEP_PIV, width), (sizes[height], SEP_PIV, width)], arrived
        )
        parent = exchange(tiles, height).reshape(-1, width)
        here, held = applied(places, couplings[height - 1], parent, inverses[height - 1])
        if height == 3:
            (here,) = call(plane_pair_body, [(2, SEP_PIV, width)], here, swap(here[2:], PLANE))
        there = swap(here, CORE)
        (spread_out,) = call(
            backward_body, [(held.shape[1], width)], held, here, there, solved[height - 1]
        )
    pieces[0] = exchange(spread_out.reshape(-1, LEAF_PIV, width), 0).sum(axis=0)
    pivot_order = jnp.concatenate(pieces, axis=0)
    return move_rows(to_slots(recv_index, pivot_order))[send_index]


def solution(mesh):
    wide = P("leaf", "front", None, None)
    in_specs = (P(AXES, None), P(AXES), P(AXES)) + (wide,) * 7
    return jax.shard_map(
        whole_solve, mesh=mesh, in_specs=in_specs, out_specs=P(AXES, None), check_vma=False
    )
```

```python
import jax
import jax.numpy as jnp
from jax import lax
from jax.experimental import pallas as pl
from jax.experimental.pallas import tpu as pltpu
from jax.sharding import PartitionSpec as P


LEAF_PIV = 384
SEP_PIV = 128
PIVOTS = (LEAF_PIV, SEP_PIV, SEP_PIV, SEP_PIV)
AXES = ("leaf", "front")
F32 = jnp.float32
BF16 = jnp.bfloat16
SLOTS = 16
CHIPS = 4
CORE = 1
PLANE = 32
VMEM = pltpu.VMEM
HBM = pltpu.HBM


def params(mib):
    return pltpu.CompilerParams(vmem_limit_bytes=mib * 2**20)


def on_chip(x):
    return pltpu.with_memory_space_constraint(x, VMEM)


def off_chip(x):
    return pltpu.with_memory_space_constraint(x, HBM)


def vmem_specs(count):
    return [pl.BlockSpec(memory_space=VMEM)] * count


def call(body, outs, *args):
    return pl.pallas_call(
        body,
        in_specs=vmem_specs(len(args)),
        out_specs=vmem_specs(len(outs)),
        out_shape=[VMEM(shape, F32) for shape in outs],
        compiler_params=params(16),
    )(*[on_chip(a) for a in args])


def same_core_groups(height):
    leaves, fronts = lax.axis_size("leaf"), lax.axis_size("front")
    span = 2**height
    return [
        [(base + leaf) * fronts + 2 * chip + core for chip in range(fronts // 2) for leaf in range(span)]
        for base in range(0, leaves, span)
        for core in range(2)
    ]


def exchange(tiles, height):
    return lax.all_to_all(
        tiles, AXES, 0, 0, axis_index_groups=same_core_groups(min(height, 2)), tiled=True
    )


def swap(block, mask):
    count = lax.axis_size("leaf") * lax.axis_size("front")
    return lax.ppermute(block, AXES, [(i, i ^ mask) for i in range(count)])


def pair_of(x):
    high = x.astype(BF16)
    return high, (x - high.astype(F32)).astype(BF16)


def dot(a, b):
    return jnp.dot(a, b, preferred_element_type=F32)


def moves(pieces, at_ref, sources, sends, stages, in_sem, out_sem):
    inward, outward = [], []
    for number, (source, cuts, place) in enumerate(pieces):
        width = stages[number].shape[1] // CHIPS
        inward.append([])
        for chip in range(CHIPS):
            block = 2 * cuts * chip + at_ref[place]
            here = pl.ds(pl.multiple_of(block * width, 128), width)
            inward[-1].append(
                pltpu.make_async_copy(
                    sources[source].at[:, here],
                    stages[number].at[:, pl.ds(chip * width, width)],
                    in_sem.at[number * CHIPS + chip],
                )
            )
        outward.append(pltpu.make_async_copy(stages[number], sends[number], out_sem.at[number]))
    return inward, outward


def cut_sends(places, matrices, pieces, owner=None, rows=None):
    shapes = [(matrices[m].shape[0], matrices[m].shape[1] // (2 * cuts)) for m, cuts, _ in pieces]
    count, total = len(pieces), len(matrices)
    extra = [] if rows is None else [owner[None, :], rows]

    def body(at_ref, *refs):
        sources, refs = refs[:total], refs[total:]
        given, refs = refs[: len(extra)], refs[len(extra) :]
        sends, refs = refs[:count], refs[count:]
        filled, refs = refs[: len(extra)], refs[len(extra) :]
        stages, sems = refs[:count], refs[count:]
        inward, outward = moves(pieces, at_ref, sources, sends, stages, *sems)
        for group in inward:
            for copy in group:
                copy.start()
        if extra:
            slots = filled[0].shape[0]
            filled[1][...] = slot_of(given[0][...])
            slots_body(filled[1], given[1], filled[0], 0, slots // 2)
        for group, after in zip(inward, outward):
            for copy in group:
                copy.wait()
            after.start()
        if extra:
            slots_body(filled[1], given[1], filled[0], slots // 2, slots)
        for copy in outward:
            copy.wait()

    peers = lax.axis_size("leaf") * lax.axis_size("front")
    slots = []
    if extra:
        slots = [VMEM((peers * SLOTS, rows.shape[1]), F32), VMEM((1, rows.shape[0]), jnp.int32)]
    return pl.pallas_call(
        body,
        in_specs=[pl.BlockSpec(memory_space=pltpu.SMEM)]
        + [pl.BlockSpec(memory_space=HBM)] * total
        + vmem_specs(len(extra)),
        out_specs=[pl.BlockSpec(memory_space=HBM)] * count + vmem_specs(len(slots)),
        out_shape=[HBM(shape, F32) for shape in shapes] + slots,
        scratch_shapes=[VMEM(shape, F32) for shape in shapes]
        + [pltpu.SemaphoreType.DMA((CHIPS * count,)), pltpu.SemaphoreType.DMA((count,))],
        compiler_params=params(20),
    )(places, *[off_chip(m) for m in matrices], *extra)


def shape_of(mats):
    return (len(mats) * mats[1].shape[0], mats[1].shape[1])


def loads(at_ref, sources, held, sem):
    parts = len(sources)
    rows, width = held.shape[0] // parts, held.shape[1] // CHIPS
    cuts = sources[0].shape[1] // (2 * CHIPS * width)

    def copy(part, step):
        there = pl.ds(pl.multiple_of(step * width, 128), width)
        block = 2 * cuts * step + at_ref[cuts - 1] if part == 0 else step
        here = pl.ds(pl.multiple_of(block * width, 128), width)
        return pltpu.make_async_copy(
            sources[part].at[:, here], held.at[pl.ds(part * rows, rows), there], sem.at[part, step]
        )

    def start():
        for step in range(CHIPS):
            for part in range(parts):
                copy(part, step).start()

    def wait(step):
        for part in range(parts):
            copy(part, step).wait()

    return start, wait


def applied(places, mats, vectors, following=None):
    parts, rows, count = len(mats), mats[1].shape[0], vectors.shape[1]
    extra = list(following or [])

    def body(at_ref, *refs):
        sources, later = refs[:parts], refs[parts : parts + len(extra)]
        vec_ref, out_ref, kept_ref = refs[parts + len(extra) : parts + len(extra) + 3]
        acc_ref, sem, late_sem, *spare = refs[parts + len(extra) + 3 :]
        held = spare[0] if extra else kept_ref
        start, wait = loads(at_ref, sources, held, sem)
        start()
        if extra:
            late_start, late_wait = loads(at_ref, later, kept_ref, late_sem)
            late_start()
        width = held.shape[1] // CHIPS
        acc_ref[...] = jnp.zeros(acc_ref.shape, F32)

        @pl.loop(0, CHIPS)
        def _(step):
            wait(step)
            at = pl.ds(pl.multiple_of(step * width, 128), width)
            high, low = pair_of(held[:, at])
            right = jnp.concatenate(pair_of(vec_ref[at, :]), axis=1)
            full = dot(high, right) + dot(low, right)
            acc_ref[...] += full[:, :count] + full[:, count:]

        for part in range(parts):
            out_ref[part] = acc_ref[part * rows : (part + 1) * rows]
        if extra:
            for step in range(CHIPS):
                late_wait(step)

    kept = shape_of(extra or mats)
    return pl.pallas_call(
        body,
        in_specs=[pl.BlockSpec(memory_space=pltpu.SMEM)]
        + [pl.BlockSpec(memory_space=HBM)] * (parts + len(extra))
        + vmem_specs(1),
        out_specs=vmem_specs(2),
        out_shape=[VMEM((parts, rows, count), F32), VMEM(kept, F32)],
        scratch_shapes=[
            VMEM((parts * rows, count), F32),
            pltpu.SemaphoreType.DMA((parts, CHIPS)),
            pltpu.SemaphoreType.DMA((max(1, len(extra)), CHIPS)),
        ]
        + ([VMEM(shape_of(mats), F32)] if extra else []),
        compiler_params=params(20),
    )(places, *[off_chip(m) for m in list(mats) + extra], on_chip(vectors))


def spread(held_ref, vector, out_ref):
    left = jnp.concatenate(pair_of(vector.T), axis=0)
    count, width = vector.shape[1], held_ref.shape[1] // CHIPS

    @pl.loop(0, CHIPS)
    def _(step):
        at = pl.ds(pl.multiple_of(step * width, 128), width)
        up, down = pair_of(held_ref[:, at])
        full = dot(left, up) + dot(left, down)
        out_ref[at, :] = (full[:count] + full[count:]).T


def rows_of(*tiles):
    return jnp.concatenate(tiles, axis=0)


def joined(here_ref, there_ref):
    return rows_of(here_ref[0] + there_ref[1], here_ref[1] + there_ref[0])


def forward_body(held_ref, here_ref, there_ref, out_ref, solved_ref):
    solved = joined(here_ref, there_ref)
    solved_ref[...] = solved
    spread(held_ref, solved, out_ref)


def plane_body(held_ref, solved_ref, far_ref, out_ref):
    spread(held_ref, rows_of(solved_ref[...], far_ref[...]), out_ref)


def top_body(held_ref, mine_ref, theirs_ref, out_ref):
    spread(held_ref, rows_of(mine_ref[0], theirs_ref[0], mine_ref[1], theirs_ref[1]), out_ref)


def backward_body(held_ref, here_ref, there_ref, solved_ref, out_ref):
    spread(held_ref, solved_ref[...] - joined(here_ref, there_ref), out_ref)


def joined_body(here_ref, there_ref, out_ref):
    out_ref[...] = joined(here_ref, there_ref)


def add_body(here_ref, there_ref, out_ref):
    out_ref[...] = here_ref[...] + there_ref[...]


def cross_body(here_ref, there_ref, out_ref):
    for part in range(2):
        out_ref[part] = here_ref[part] + there_ref[1 - part]


def plane_pair_body(here_ref, there_ref, out_ref):
    for part in range(2):
        out_ref[part] = here_ref[part] + there_ref[part]


def minus_sum_body(tiles_ref, base_ref, out_ref):
    share = base_ref[...] - jnp.sum(tiles_ref[...], axis=0)
    out_ref[...] = jnp.broadcast_to(share[None], out_ref.shape)


def sum_body(tiles_ref, share_ref, out_ref):
    share = jnp.sum(tiles_ref[...], axis=0)
    share_ref[...] = share
    out_ref[...] = jnp.broadcast_to(share[None], out_ref.shape)


def slot_of(owner):
    count = owner.shape[1]
    target = jnp.floor((owner.astype(F32) + 0.5) * (1.0 / count))
    down = jnp.broadcast_to(target, (8, count)).T[:, :1]
    earlier = lax.broadcasted_iota(jnp.int32, (count, count), 0) < lax.broadcasted_iota(
        jnp.int32, (count, count), 1
    )
    rank = jnp.sum(jnp.where((down == target) & earlier, 1.0, 0.0), axis=0, keepdims=True)
    return (target * SLOTS + rank).astype(jnp.int32)


def slots_body(index_ref, rows_ref, out_ref, first, last):
    parts = jnp.concatenate(pair_of(rows_ref[...]), axis=1)
    count, width = rows_ref.shape
    index = index_ref[...]

    @pl.loop(first // 512, last // 512)
    def _(step):
        start = pl.multiple_of(step * 512, 512)
        slot = lax.broadcasted_iota(jnp.int32, (512, count), 0) + start
        chosen = dot((slot == index).astype(F32).astype(BF16), parts)
        out_ref[pl.ds(start, 512), :] = chosen[:, :width] + chosen[:, width:]


def to_slots(index, rows):
    peers = lax.axis_size("leaf") * lax.axis_size("front")
    return pl.pallas_call(
        lambda *refs: slots_body(*refs, 0, peers * SLOTS),
        in_specs=vmem_specs(2),
        out_specs=pl.BlockSpec(memory_space=VMEM),
        out_shape=VMEM((peers * SLOTS, rows.shape[1]), F32),
        compiler_params=params(16),
    )(index[None, :], rows)


def rank_among(keys, order):
    same = (keys[:, None] == keys[None, :]) & (order[None, :] < order[:, None])
    return jnp.sum(same.astype(jnp.int32), axis=1)


def move_rows(outgoing):
    tiles = outgoing.reshape(-1, SLOTS, outgoing.shape[1])
    return lax.all_to_all(tiles, AXES, 0, 0, tiled=True).reshape(outgoing.shape)


def whole_solve(app_rhs, pivot_source, row_owner, *matrices):
    core = lax.axis_index("front") % 2
    plane = lax.axis_index("leaf") // 4 % 2
    row_count, width = app_rhs.shape
    matrices = [m[0, 0] for m in matrices]

    anchor = pivot_source // row_count
    recv_index = anchor * SLOTS + rank_among(anchor, pivot_source)

    def all_places(core, plane):
        near, far = 2 * core + plane, 2 * (1 - core) + plane
        table = [core, near, 1 - core, far, near + 1 - 2 * plane, far + 1 - 2 * plane]
        return jnp.stack(table).astype(jnp.int32)

    places = all_places(core, plane)
    first = [(0, 1, 2), (1, 1, 2)]
    *sends, outgoing, send_index = cut_sends(places, matrices[:2], first, row_owner, app_rhs)
    mats = [[matrices[m], swap(sends[m], CORE)] for m in range(2)]
    ordered = move_rows(outgoing)[recv_index]
    ordered, core, plane = lax.optimization_barrier((ordered, core, plane))
    late = [(0, 1, 2), (1, 1, 2)] + [(m, 2, p) for m in (2, 3) for p in (4, 5)]
    sends = cut_sends(all_places(core, plane), matrices[2:4] + matrices[5:], late)
    mats += [[matrices[m], swap(sends[m - 2], CORE)] for m in (2, 3)]
    far = []
    for number, piece in enumerate(range(2, 6)):
        half = swap(sends[piece], (PLANE, PLANE | CORE)[number % 2])
        far.append(half)
    starts = (0, LEAF_PIV, LEAF_PIV + SEP_PIV, LEAF_PIV + 2 * SEP_PIV)
    sizes = (CHIPS, 2 * CHIPS, 4 * CHIPS, 4 * CHIPS)
    own = [ordered[at : at + rows] for at, rows in zip(starts, PIVOTS)]
    tiles = jnp.broadcast_to(own[0][None], (sizes[0], LEAF_PIV, width))
    solved = []
    for height in range(3):
        gathered = exchange(tiles, height).reshape(-1, width)
        here, held = applied(places, mats[2 * height], gathered, mats[2 * height + 1])
        there = swap(here, CORE)
        outs = [(held.shape[1], width), (2 * PIVOTS[height], width)]
        if height < 2:
            carried, forward = call(forward_body, outs, held, here, there)
            if height == 0:
                carried, core, plane = lax.optimization_barrier((carried, core, plane))
                late = [(0, 1, 2), (1, 2, 3), (2, 2, 3)]
                sends = cut_sends(all_places(core, plane), matrices[4:], late)
                for m in range(4, 7):
                    mats.append([matrices[m], swap(sends[m - 4], CORE)])
                mats[5] += far[:2]
                mats[6] += far[2:]
        else:
            (forward,) = call(joined_body, outs[1:], here, there)
            (carried,) = call(plane_body, outs[:1], held, forward, swap(forward, PLANE))
        solved.append(forward)
        arrived = exchange(carried.reshape(-1, SEP_PIV, width), height + 1)
        (tiles,) = call(
            minus_sum_body, [(sizes[height + 1], SEP_PIV, width)], arrived, own[height + 1]
        )
    here, held = applied(places, mats[6], exchange(tiles, 3).reshape(-1, width))
    mine, theirs = here[0::2], here[1::2]
    (mine,) = call(add_body, [mine.shape], mine, swap(theirs, CORE))
    (mine,) = call(cross_body, [mine.shape], mine, swap(mine, PLANE))
    (spread_out,) = call(top_body, [(held.shape[1], width)], held, mine, swap(mine, CORE))
    pieces = [None, None, None, None]
    for height in (3, 2, 1):
        arrived = exchange(spread_out.reshape(-1, SEP_PIV, width), height)
        pieces[height], tiles = call(
            sum_body, [(SEP_PIV, width), (sizes[height], SEP_PIV, width)], arrived
        )
        parent = exchange(tiles, height).reshape(-1, width)
        here, held = applied(places, mats[2 * height - 1], parent, mats[2 * height - 2])
        if height == 3:
            (here,) = call(plane_pair_body, [(2, SEP_PIV, width)], here, swap(here[2:], PLANE))
        there = swap(here, CORE)
        (spread_out,) = call(
            backward_body, [(held.shape[1], width)], held, here, there, solved[height - 1]
        )
    pieces[0] = exchange(spread_out.reshape(-1, LEAF_PIV, width), 0).sum(axis=0)
    pivot_order = jnp.concatenate(pieces, axis=0)
    return move_rows(to_slots(recv_index, pivot_order))[send_index[0]]


def solution(mesh):
    wide = P("leaf", "front", None, None)
    in_specs = (P(AXES, None), P(AXES), P(AXES)) + (wide,) * 7
    return jax.shard_map(
        whole_solve, mesh=mesh, in_specs=in_specs, out_specs=P(AXES, None), check_vma=False
    )
```

```python
import jax
import jax.numpy as jnp
from jax import lax
from jax.experimental import pallas as pl
from jax.experimental.pallas import tpu as pltpu
from jax.sharding import PartitionSpec as P


LEAF_PIV = 384
SEP_PIV = 128
PIVOTS = (LEAF_PIV, SEP_PIV, SEP_PIV, SEP_PIV)
AXES = ("leaf", "front")
F32 = jnp.float32
BF16 = jnp.bfloat16
SLOTS = 16
CHIPS = 4
CORE = 1
PLANE = 32
VMEM = pltpu.VMEM
HBM = pltpu.HBM


def params(mib):
    return pltpu.CompilerParams(vmem_limit_bytes=mib * 2**20)


def on_chip(x):
    return pltpu.with_memory_space_constraint(x, VMEM)


def off_chip(x):
    return pltpu.with_memory_space_constraint(x, HBM)


def vmem_specs(count):
    return [pl.BlockSpec(memory_space=VMEM)] * count


def call(body, outs, *args):
    return pl.pallas_call(
        body,
        in_specs=vmem_specs(len(args)),
        out_specs=vmem_specs(len(outs)),
        out_shape=[VMEM(shape, F32) for shape in outs],
        compiler_params=params(16),
    )(*[on_chip(a) for a in args])


def same_core_groups(height):
    leaves, fronts = lax.axis_size("leaf"), lax.axis_size("front")
    span = 2**height
    return [
        [(base + leaf) * fronts + 2 * chip + core for chip in range(fronts // 2) for leaf in range(span)]
        for base in range(0, leaves, span)
        for core in range(2)
    ]


def exchange(tiles, height):
    return lax.all_to_all(
        tiles, AXES, 0, 0, axis_index_groups=same_core_groups(min(height, 2)), tiled=True
    )


def swap(block, mask):
    count = lax.axis_size("leaf") * lax.axis_size("front")
    return lax.ppermute(block, AXES, [(i, i ^ mask) for i in range(count)])


def pair_of(x):
    high = x.astype(BF16)
    return high, (x - high.astype(F32)).astype(BF16)


def dot(a, b):
    return jnp.dot(a, b, preferred_element_type=F32)


def moves(pieces, at_ref, sources, sends, stages, in_sem, out_sem):
    inward, outward = [], []
    for number, (source, cuts, place) in enumerate(pieces):
        width = stages[number].shape[1] // CHIPS
        inward.append([])
        for chip in range(CHIPS):
            block = 2 * cuts * chip + at_ref[place]
            here = pl.ds(pl.multiple_of(block * width, 128), width)
            inward[-1].append(
                pltpu.make_async_copy(
                    sources[source].at[:, here],
                    stages[number].at[:, pl.ds(chip * width, width)],
                    in_sem.at[number * CHIPS + chip],
                )
            )
        outward.append(pltpu.make_async_copy(stages[number], sends[number], out_sem.at[number]))
    return inward, outward


def cut_sends(places, matrices, pieces, owner=None, rows=None):
    shapes = [(matrices[m].shape[0], matrices[m].shape[1] // (2 * cuts)) for m, cuts, _ in pieces]
    count, total = len(pieces), len(matrices)
    extra = [] if rows is None else [owner[None, :], rows]

    def body(at_ref, *refs):
        sources, refs = refs[:total], refs[total:]
        given, refs = refs[: len(extra)], refs[len(extra) :]
        sends, refs = refs[:count], refs[count:]
        filled, refs = refs[: len(extra)], refs[len(extra) :]
        stages, sems = refs[:count], refs[count:]
        inward, outward = moves(pieces, at_ref, sources, sends, stages, *sems)
        for group in inward:
            for copy in group:
                copy.start()
        if extra:
            slots = filled[0].shape[0]
            filled[1][...] = slot_of(given[0][...])
            slots_body(filled[1], given[1], filled[0], 0, slots // 2)
        for group, after in zip(inward, outward):
            for copy in group:
                copy.wait()
            after.start()
        if extra:
            slots_body(filled[1], given[1], filled[0], slots // 2, slots)
        for copy in outward:
            copy.wait()

    peers = lax.axis_size("leaf") * lax.axis_size("front")
    slots = []
    if extra:
        slots = [VMEM((peers * SLOTS, rows.shape[1]), F32), VMEM((1, rows.shape[0]), jnp.int32)]
    return pl.pallas_call(
        body,
        in_specs=[pl.BlockSpec(memory_space=pltpu.SMEM)]
        + [pl.BlockSpec(memory_space=HBM)] * total
        + vmem_specs(len(extra)),
        out_specs=[pl.BlockSpec(memory_space=HBM)] * count + vmem_specs(len(slots)),
        out_shape=[HBM(shape, F32) for shape in shapes] + slots,
        scratch_shapes=[VMEM(shape, F32) for shape in shapes]
        + [pltpu.SemaphoreType.DMA((CHIPS * count,)), pltpu.SemaphoreType.DMA((count,))],
        compiler_params=params(20),
    )(places, *[off_chip(m) for m in matrices], *extra)


def shape_of(mats):
    return (len(mats) * mats[1].shape[0], mats[1].shape[1])


def loads(at_ref, sources, held, sem):
    parts = len(sources)
    rows, width = held.shape[0] // parts, held.shape[1] // CHIPS
    cuts = sources[0].shape[1] // (2 * CHIPS * width)

    def copy(part, step):
        there = pl.ds(pl.multiple_of(step * width, 128), width)
        block = 2 * cuts * step + at_ref[cuts - 1] if part == 0 else step
        here = pl.ds(pl.multiple_of(block * width, 128), width)
        return pltpu.make_async_copy(
            sources[part].at[:, here], held.at[pl.ds(part * rows, rows), there], sem.at[part, step]
        )

    def start():
        for step in range(CHIPS):
            for part in range(parts):
                copy(part, step).start()

    def wait(step):
        for part in range(parts):
            copy(part, step).wait()

    return start, wait


def applied(places, mats, vectors, following=None):
    parts, rows, count = len(mats), mats[1].shape[0], vectors.shape[1]
    extra = list(following or [])

    def body(at_ref, *refs):
        sources, later = refs[:parts], refs[parts : parts + len(extra)]
        vec_ref, out_ref, kept_ref = refs[parts + len(extra) : parts + len(extra) + 3]
        acc_ref, sem, late_sem, *spare = refs[parts + len(extra) + 3 :]
        held = spare[0] if extra else kept_ref
        start, wait = loads(at_ref, sources, held, sem)
        start()
        if extra:
            late_start, late_wait = loads(at_ref, later, kept_ref, late_sem)
            late_start()
        width = held.shape[1] // CHIPS
        acc_ref[...] = jnp.zeros(acc_ref.shape, F32)

        @pl.loop(0, CHIPS)
        def _(step):
            wait(step)
            at = pl.ds(pl.multiple_of(step * width, 128), width)
            high, low = pair_of(held[:, at])
            right = jnp.concatenate(pair_of(vec_ref[at, :]), axis=1)
            full = dot(high, right) + dot(low, right)
            acc_ref[...] += full[:, :count] + full[:, count:]

        for part in range(parts):
            out_ref[part] = acc_ref[part * rows : (part + 1) * rows]
        if extra:
            for step in range(CHIPS):
                late_wait(step)

    kept = shape_of(extra or mats)
    return pl.pallas_call(
        body,
        in_specs=[pl.BlockSpec(memory_space=pltpu.SMEM)]
        + [pl.BlockSpec(memory_space=HBM)] * (parts + len(extra))
        + vmem_specs(1),
        out_specs=vmem_specs(2),
        out_shape=[VMEM((parts, rows, count), F32), VMEM(kept, F32)],
        scratch_shapes=[
            VMEM((parts * rows, count), F32),
            pltpu.SemaphoreType.DMA((parts, CHIPS)),
            pltpu.SemaphoreType.DMA((max(1, len(extra)), CHIPS)),
        ]
        + ([VMEM(shape_of(mats), F32)] if extra else []),
        compiler_params=params(20),
    )(places, *[off_chip(m) for m in list(mats) + extra], on_chip(vectors))


def spread(held_ref, vector, out_ref):
    left = jnp.concatenate(pair_of(vector.T), axis=0)
    count, width = vector.shape[1], held_ref.shape[1] // CHIPS

    @pl.loop(0, CHIPS)
    def _(step):
        at = pl.ds(pl.multiple_of(step * width, 128), width)
        up, down = pair_of(held_ref[:, at])
        full = dot(left, up) + dot(left, down)
        out_ref[at, :] = (full[:count] + full[count:]).T


def rows_of(*tiles):
    return jnp.concatenate(tiles, axis=0)


def joined(here_ref, there_ref):
    return rows_of(here_ref[0] + there_ref[1], here_ref[1] + there_ref[0])


def forward_body(held_ref, here_ref, there_ref, out_ref, solved_ref):
    solved = joined(here_ref, there_ref)
    solved_ref[...] = solved
    spread(held_ref, solved, out_ref)


def plane_body(held_ref, solved_ref, far_ref, out_ref):
    spread(held_ref, rows_of(solved_ref[...], far_ref[...]), out_ref)


def top_body(held_ref, mine_ref, theirs_ref, out_ref):
    spread(held_ref, rows_of(mine_ref[0], theirs_ref[0], mine_ref[1], theirs_ref[1]), out_ref)


def backward_body(held_ref, here_ref, there_ref, solved_ref, out_ref):
    spread(held_ref, solved_ref[...] - joined(here_ref, there_ref), out_ref)


def leaf_body(chip_ref, held_ref, here_ref, there_ref, solved_ref, *outs):
    vector = solved_ref[...] - joined(here_ref, there_ref)
    left = jnp.concatenate(pair_of(vector.T), axis=0)
    count, width = vector.shape[1], held_ref.shape[1] // CHIPS
    for turn, out_ref in enumerate(outs):
        block = lax.rem(chip_ref[0] + turn, CHIPS)
        up, down = pair_of(held_ref[:, pl.ds(pl.multiple_of(block * width, 128), width)])
        full = dot(left, up) + dot(left, down)
        out_ref[...] = (full[:count] + full[count:]).T


def leaf_sum(chip, held, here, there, solved):
    shape = (held.shape[1] // CHIPS, here.shape[2])
    parts = pl.pallas_call(
        leaf_body,
        in_specs=[pl.BlockSpec(memory_space=pltpu.SMEM)] + vmem_specs(4),
        out_specs=vmem_specs(CHIPS),
        out_shape=[VMEM(shape, F32)] * CHIPS,
        compiler_params=params(16),
    )(chip.reshape(1), *[on_chip(a) for a in (held, here, there, solved)])
    fronts = lax.axis_size("front")
    count = lax.axis_size("leaf") * fronts
    total = parts[0]
    for turn in (1, 3, 2):
        route = [(i, i - i % fronts + (i + 2 * turn) % fronts) for i in range(count)]
        total = total + lax.ppermute(parts[turn], AXES, route)
    return total


def joined_body(here_ref, there_ref, out_ref):
    out_ref[...] = joined(here_ref, there_ref)


def add_body(here_ref, there_ref, out_ref):
    out_ref[...] = here_ref[...] + there_ref[...]


def cross_body(here_ref, there_ref, out_ref):
    for part in range(2):
        out_ref[part] = here_ref[part] + there_ref[1 - part]


def plane_pair_body(here_ref, there_ref, out_ref):
    for part in range(2):
        out_ref[part] = here_ref[part] + there_ref[part]


def minus_sum_body(tiles_ref, base_ref, out_ref):
    share = base_ref[...] - jnp.sum(tiles_ref[...], axis=0)
    out_ref[...] = jnp.broadcast_to(share[None], out_ref.shape)


def sum_body(tiles_ref, share_ref, out_ref):
    share = jnp.sum(tiles_ref[...], axis=0)
    share_ref[...] = share
    out_ref[...] = jnp.broadcast_to(share[None], out_ref.shape)


def slot_of(owner):
    count = owner.shape[1]
    target = jnp.floor((owner.astype(F32) + 0.5) * (1.0 / count))
    down = jnp.broadcast_to(target, (8, count)).T[:, :1]
    earlier = lax.broadcasted_iota(jnp.int32, (count, count), 0) < lax.broadcasted_iota(
        jnp.int32, (count, count), 1
    )
    rank = jnp.sum(jnp.where((down == target) & earlier, 1.0, 0.0), axis=0, keepdims=True)
    return (target * SLOTS + rank).astype(jnp.int32)


def slots_body(index_ref, rows_ref, out_ref, first, last):
    parts = jnp.concatenate(pair_of(rows_ref[...]), axis=1)
    count, width = rows_ref.shape
    index = index_ref[...]

    @pl.loop(first // 512, last // 512)
    def _(step):
        start = pl.multiple_of(step * 512, 512)
        slot = lax.broadcasted_iota(jnp.int32, (512, count), 0) + start
        chosen = dot((slot == index).astype(F32).astype(BF16), parts)
        out_ref[pl.ds(start, 512), :] = chosen[:, :width] + chosen[:, width:]


def to_slots(index, rows):
    peers = lax.axis_size("leaf") * lax.axis_size("front")
    return pl.pallas_call(
        lambda *refs: slots_body(*refs, 0, peers * SLOTS),
        in_specs=vmem_specs(2),
        out_specs=pl.BlockSpec(memory_space=VMEM),
        out_shape=VMEM((peers * SLOTS, rows.shape[1]), F32),
        compiler_params=params(16),
    )(index[None, :], rows)


def rank_among(keys, order):
    same = (keys[:, None] == keys[None, :]) & (order[None, :] < order[:, None])
    return jnp.sum(same.astype(jnp.int32), axis=1)


def move_rows(outgoing):
    tiles = outgoing.reshape(-1, SLOTS, outgoing.shape[1])
    return lax.all_to_all(tiles, AXES, 0, 0, tiled=True).reshape(outgoing.shape)


def whole_solve(app_rhs, pivot_source, row_owner, *matrices):
    core = lax.axis_index("front") % 2
    plane = lax.axis_index("leaf") // 4 % 2
    row_count, width = app_rhs.shape
    matrices = [m[0, 0] for m in matrices]

    anchor = pivot_source // row_count
    recv_index = anchor * SLOTS + rank_among(anchor, pivot_source)

    def all_places(core, plane):
        near, far = 2 * core + plane, 2 * (1 - core) + plane
        table = [core, near, 1 - core, far, near + 1 - 2 * plane, far + 1 - 2 * plane]
        return jnp.stack(table).astype(jnp.int32)

    places = all_places(core, plane)
    first = [(0, 1, 2), (1, 1, 2)]
    *sends, outgoing, send_index = cut_sends(places, matrices[:2], first, row_owner, app_rhs)
    mats = [[matrices[m], swap(sends[m], CORE)] for m in range(2)]
    ordered = move_rows(outgoing)[recv_index]
    ordered, core, plane = lax.optimization_barrier((ordered, core, plane))
    late = [(0, 1, 2), (1, 1, 2)] + [(m, 2, p) for m in (2, 3) for p in (4, 5)]
    sends = cut_sends(all_places(core, plane), matrices[2:4] + matrices[5:], late)
    mats += [[matrices[m], swap(sends[m - 2], CORE)] for m in (2, 3)]
    far = []
    for number, piece in enumerate(range(2, 6)):
        half = swap(sends[piece], (PLANE, PLANE | CORE)[number % 2])
        far.append(half)
    starts = (0, LEAF_PIV, LEAF_PIV + SEP_PIV, LEAF_PIV + 2 * SEP_PIV)
    sizes = (CHIPS, 2 * CHIPS, 4 * CHIPS, 4 * CHIPS)
    own = [ordered[at : at + rows] for at, rows in zip(starts, PIVOTS)]
    tiles = jnp.broadcast_to(own[0][None], (sizes[0], LEAF_PIV, width))
    solved = []
    for height in range(3):
        gathered = exchange(tiles, height).reshape(-1, width)
        here, held = applied(places, mats[2 * height], gathered, mats[2 * height + 1])
        there = swap(here, CORE)
        outs = [(held.shape[1], width), (2 * PIVOTS[height], width)]
        if height < 2:
            carried, forward = call(forward_body, outs, held, here, there)
            if height == 0:
                carried, core, plane = lax.optimization_barrier((carried, core, plane))
                late = [(0, 1, 2), (1, 2, 3), (2, 2, 3)]
                sends = cut_sends(all_places(core, plane), matrices[4:], late)
                for m in range(4, 7):
                    mats.append([matrices[m], swap(sends[m - 4], CORE)])
                mats[5] += far[:2]
                mats[6] += far[2:]
        else:
            (forward,) = call(joined_body, outs[1:], here, there)
            (carried,) = call(plane_body, outs[:1], held, forward, swap(forward, PLANE))
        solved.append(forward)
        arrived = exchange(carried.reshape(-1, SEP_PIV, width), height + 1)
        (tiles,) = call(
            minus_sum_body, [(sizes[height + 1], SEP_PIV, width)], arrived, own[height + 1]
        )
    here, held = applied(places, mats[6], exchange(tiles, 3).reshape(-1, width))
    mine, theirs = here[0::2], here[1::2]
    (mine,) = call(add_body, [mine.shape], mine, swap(theirs, CORE))
    (mine,) = call(cross_body, [mine.shape], mine, swap(mine, PLANE))
    (spread_out,) = call(top_body, [(held.shape[1], width)], held, mine, swap(mine, CORE))
    pieces = [None, None, None, None]
    for height in (3, 2, 1):
        arrived = exchange(spread_out.reshape(-1, SEP_PIV, width), height)
        pieces[height], tiles = call(
            sum_body, [(SEP_PIV, width), (sizes[height], SEP_PIV, width)], arrived
        )
        parent = exchange(tiles, height).reshape(-1, width)
        here, held = applied(places, mats[2 * height - 1], parent, mats[2 * height - 2])
        if height == 3:
            (here,) = call(plane_pair_body, [(2, SEP_PIV, width)], here, swap(here[2:], PLANE))
        there = swap(here, CORE)
        if height > 1:
            outs = [(held.shape[1], width)]
            (spread_out,) = call(backward_body, outs, held, here, there, solved[height - 1])
    chip = lax.axis_index("front") // 2
    pieces[0] = leaf_sum(chip, held, here, there, solved[0])
    pivot_order = jnp.concatenate(pieces, axis=0)
    return move_rows(to_slots(recv_index, pivot_order))[send_index[0]]


def solution(mesh):
    wide = P("leaf", "front", None, None)
    in_specs = (P(AXES, None), P(AXES), P(AXES)) + (wide,) * 7
    return jax.shard_map(
        whole_solve, mesh=mesh, in_specs=in_specs, out_specs=P(AXES, None), check_vma=False
    )
```
